32 devices in a mesh: groups: 2 (over y), ctx: 4 (over z), head: 2 (over x), rep: 2 (over core).
Axes of the slice: x: 2, y: 2, z: 4, core: 2. Of those that a mesh axis runs over, the one named last changes fastest.
Arguments:
- queries: bfloat16 [2048, 4096], P(('groups', 'ctx'), ('head', 'rep')), parts along dimension 0, may hold values from -24 to 24
- keys: bfloat16 [2048, 1024], P(('groups', 'ctx'), ('head', 'rep')), parts along dimension 0, may hold values from -6 to 6
- values: bfloat16 [2048, 1024], P(('groups', 'ctx'), ('head', 'rep')), parts along dimension 0, may hold values from -6 to 6
- span_order: int32 [8], replicated, may hold values from 0 to 7, as said below
Outputs:
- attended: bfloat16 [2048, 4096], P(('groups', 'ctx'), ('head', 'rep')), parts along dimension 0
The draws below stay inside these ranges and needn't reach their ends.
There are 2 independent parts, one for each index of `groups`. The reference program is written for one: setup_inputs(seed, part) draws one part's arguments, and reference() takes and returns one part's arrays. A program takes and returns all parts, laid end to end along the dimension named above; an argument that names none is the same for every part. Nothing has to cross between parts.
Inputs may be any that keep to these rules, and one draw needn't show every extreme that they name: `span_order`: A permutation of the spans in which entries 2 d and 2 d + 1 are c and 7 - c for some c.
All inputs are finite; a program needn't handle non-finite values.
Results may differ from the reference program's by a relative error of at most 0.0047.
Values may be sent and summed in bfloat16 or wider, within the bound.
No kernel may reach another device: no remote copies, remote signals or barrier semaphores. Data moves between devices by JAX's collectives and lax.ppermute only.
A program may use at most 64 MiB of HBM per device.

```python
import math
import jax
import jax.numpy as jnp
from jax import lax

QUERY_HEADS = 32
KEY_VALUE_HEADS = 8
HEAD_SIZE = 128
SPAN = 128
SPANS = 8
SEQUENCE_TOKENS = 1024


def draw_queries(key, part):
    perturb_random_key = jax.random.fold_in(key, 21)
    scale_key = jax.random.fold_in(key, 22)
    noise = jax.random.truncated_normal(perturb_random_key, -4.0, 4.0, (SEQUENCE_TOKENS, QUERY_HEADS, HEAD_SIZE), jnp.float32)
    row_scale = jnp.exp(jax.random.uniform(scale_key, (SEQUENCE_TOKENS, QUERY_HEADS, 1), jnp.float32, 0.0, math.log(6.0)))
    sampled_values = noise * row_scale
    return sampled_values.reshape(SEQUENCE_TOKENS, QUERY_HEADS * HEAD_SIZE).astype(jnp.bfloat16)


def draw_keys(key, part):
    perturb_random_key = jax.random.fold_in(key, 31)
    sampled_values = jax.random.truncated_normal(perturb_random_key, -6.0, 6.0, (SEQUENCE_TOKENS, KEY_VALUE_HEADS, HEAD_SIZE), jnp.float32)
    return sampled_values.reshape(SEQUENCE_TOKENS, KEY_VALUE_HEADS * HEAD_SIZE).astype(jnp.bfloat16)


def draw_span_order(key, part):
    pair_count = SPANS // 2
    pair_order = jax.random.permutation(jax.random.fold_in(key, 41), pair_count)
    flip_bits = jax.random.randint(jax.random.fold_in(key, 42), (pair_count,), 0, 2)
    first_span = jnp.where(flip_bits == 1, pair_order, SPANS - 1 - pair_order)
    second_span = SPANS - 1 - first_span
    return jnp.stack([first_span, second_span], axis=1).reshape(SPANS).astype(jnp.int32)


def block_levels(key, extent, pieces, low, high):
    factor_of = 1.0
    for axis_at, blocks in pieces:
        steps = jax.random.uniform(jax.random.fold_in(jax.random.fold_in(key, 6), axis_at), (blocks,), jnp.float32, low / len(pieces), high / len(pieces))
        factor_of = factor_of * jnp.repeat(jnp.exp(steps), extent[axis_at] // blocks).reshape((-1,) + (1,) * (len(extent) - 1 - axis_at))
    return factor_of


def bell_draw(stream_key, shape, scale, most, cuts=(), kind=jnp.bfloat16):
    result = jax.random.normal(stream_key, shape, jnp.float32) * scale
    if len(cuts) > 0:
        result = block_levels(stream_key, shape, cuts, -0.22, 0.18) * result
    return jnp.clip(result, min=-most, max=most).astype(kind)


def setup_inputs(seed: int = 0, part: int = 0) -> dict:
    arg_keys = jax.random.split(jax.random.key(seed), 5)
    part_keys = jax.random.split(jax.random.fold_in(arg_keys[4], part), 5)
    queries = draw_queries(jax.random.fold_in(jax.random.fold_in(arg_keys[4], part), 71), part)
    keys = draw_keys(jax.random.fold_in(jax.random.fold_in(arg_keys[4], part), 71), part)
    values = bell_draw(part_keys[2], (SEQUENCE_TOKENS, KEY_VALUE_HEADS * HEAD_SIZE), 1.0, 6.0, ((0, 4), (1, 4)))
    span_order = draw_span_order(jax.random.fold_in(arg_keys[4], 71), part)
    return {"queries": queries, "keys": keys, "values": values, "span_order": span_order}


masked_score = -1e+30

def source_partials(query_block, query_pos, key_block, value_block, key_pos):
    score_scale = 1.0 / math.sqrt(HEAD_SIZE)
    scores = jnp.einsum('rhgd,shd->rhgs', query_block, key_block) * score_scale
    allowed = (key_pos[None, :] <= query_pos[:, None])[:, None, None, :]
    masked = jnp.where(allowed, scores, masked_score)
    row_top = lax.optimization_barrier(jnp.max(masked, axis=-1))
    weights = jnp.where(allowed, jnp.exp(masked - row_top[..., None]), 0.0)
    row_total = lax.optimization_barrier(jnp.sum(weights, axis=-1))
    rounded = lax.optimization_barrier(weights.astype(jnp.bfloat16)).astype(jnp.float32)
    numerator = jnp.einsum('rhgs,shd->rhgd', rounded, value_block)
    partial_value = numerator / jnp.maximum(row_total, 1.0)[..., None]
    partial_value = lax.optimization_barrier(partial_value.astype(jnp.bfloat16)).astype(jnp.float32)
    return (partial_value, row_top, row_total)

def reference(queries, keys, values, span_order):
    row_index = jnp.arange(SEQUENCE_TOKENS, dtype=jnp.int32)
    positions = span_order[row_index // SPAN].astype(jnp.int32) * SPAN + row_index % SPAN
    contributor_list = SPANS // 2
    rows_per_block = 2 * SPAN
    common_values = QUERY_HEADS // KEY_VALUE_HEADS
    query_block_list = queries.astype(jnp.float32).reshape(contributor_list, rows_per_block, KEY_VALUE_HEADS, common_values, HEAD_SIZE)
    key_block_list = keys.astype(jnp.float32).reshape(contributor_list, rows_per_block, KEY_VALUE_HEADS, HEAD_SIZE)
    value_block_list = values.astype(jnp.float32).reshape(contributor_list, rows_per_block, KEY_VALUE_HEADS, HEAD_SIZE)
    position_blocks = positions.reshape(contributor_list, rows_per_block)

    def one_block(operands):
        query_block, query_pos = operands

        def one_source(inputs_now):
            return source_partials(query_block, query_pos, inputs_now[0], inputs_now[1], inputs_now[2])
        partials, row_tops, row_totals = lax.map(one_source, (key_block_list, value_block_list, position_blocks))
        best_top = lax.optimization_barrier(jnp.max(row_tops, axis=0))
        source_weight = row_totals * jnp.exp(row_tops - best_top[None])
        weighted = lax.optimization_barrier(jnp.sum(source_weight[..., None] * partials, axis=0))
        return (weighted / lax.optimization_barrier(jnp.sum(source_weight, axis=0))[..., None]).astype(jnp.bfloat16)
    attended = lax.map(one_block, (query_block_list, position_blocks))
    return attended.reshape(SEQUENCE_TOKENS, QUERY_HEADS * HEAD_SIZE)
```

```python
import math

import jax
import jax.numpy as jnp
from jax import lax
from jax.experimental import pallas as pl
from jax.experimental.pallas import tpu as pltpu
from jax.sharding import PartitionSpec as P

HEAD_SIZE = 128
LOW = -1e29
MASKED = -1e30


def attend_kernel(span_rows, group, plan, has_state, last, *refs):
    span_order, q_ref = refs[:2]
    at = 2
    pieces = []
    for _ in plan:
        pieces.append((refs[at], refs[at + 1]))
        at += 2
    if has_state:
        acc_in, stat_in = refs[at : at + 2]
        at += 2
    outs = refs[at:]
    rows = q_ref.shape[0]
    heads = q_ref.shape[1] // HEAD_SIZE
    me = lax.axis_index("ctx")
    factor = math.log2(math.e) / math.sqrt(HEAD_SIZE)

    def span_pos(source, shape, axis):
        ids = lax.broadcasted_iota(jnp.int32, shape, axis)
        first = span_order[2 * source] * span_rows
        second = (span_order[2 * source + 1] - 1) * span_rows
        return ids + jnp.where(ids < span_rows, first, second)

    q_pos = span_pos(me, (1, rows), 1)
    allowed = []
    for source_of in plan:
        source, valid = source_of(me)
        k_pos = span_pos(source, (rows, 1), 0)
        if valid is not None:
            k_pos = jnp.where(valid, k_pos, jnp.int32(2**30))
        allowed.append(k_pos <= q_pos)
    for h in range(heads):
        cols = slice(h * HEAD_SIZE, (h + 1) * HEAD_SIZE)
        kv_cols = slice(h // group * HEAD_SIZE, (h // group + 1) * HEAD_SIZE)
        if has_state:
            acc = acc_in[cols, :]
            top = stat_in[h : h + 1, :]
            total = stat_in[heads + h : heads + h + 1, :]
        else:
            acc = None
        for (k_ref, v_ref), ok in zip(pieces, allowed):
            scores = lax.dot_general(
                k_ref[:, kv_cols],
                q_ref[:, cols],
                (((1,), (1,)), ((), ())),
                preferred_element_type=jnp.float32,
            )
            masked = jnp.where(ok, scores, MASKED)
            piece_top = jnp.maximum(jnp.max(masked, axis=0, keepdims=True), LOW)
            weights = jnp.exp2((masked - piece_top) * factor)
            piece_total = jnp.sum(weights, axis=0, keepdims=True)
            piece_sum = lax.dot_general(
                v_ref[:, kv_cols],
                weights.astype(jnp.bfloat16),
                (((0,), (0,)), ((), ())),
                preferred_element_type=jnp.float32,
            )
            if acc is None:
                acc, top, total = piece_sum, piece_top, piece_total
            else:
                new_top = jnp.maximum(top, piece_top)
                keep = jnp.exp2((top - new_top) * factor)
                add = jnp.exp2((piece_top - new_top) * factor)
                acc = acc * keep + piece_sum * add
                total = total * keep + piece_total * add
                top = new_top
        if last:
            outs[0][:, cols] = (acc / total).T.astype(jnp.bfloat16)
        else:
            outs[0][cols, :] = acc
            outs[1][h : h + 1, :] = top
            outs[1][heads + h : heads + h + 1, :] = total


def attend(span_order, q, pieces, plan, state, last):
    rows, width = q.shape
    heads = width // HEAD_SIZE
    group = width // pieces[0][0].shape[1]
    vmem = pl.BlockSpec(memory_space=pltpu.VMEM)
    operands = [span_order, q]
    specs = [pl.BlockSpec(memory_space=pltpu.SMEM), vmem]
    for k, v in pieces:
        operands += [k, v]
        specs += [vmem, vmem]
    if state is not None:
        operands += list(state)
        specs += [vmem, vmem]
    if last:
        out_shape = jax.ShapeDtypeStruct((rows, width), jnp.bfloat16)
        out_specs = vmem
    else:
        out_shape = (
            jax.ShapeDtypeStruct((width, rows), jnp.float32),
            jax.ShapeDtypeStruct((2 * heads, rows), jnp.float32),
        )
        out_specs = (vmem, vmem)

    def body(*refs):
        attend_kernel(rows // 2, group, plan, state is not None, last, *refs)

    return pl.pallas_call(
        body,
        out_shape=out_shape,
        in_specs=specs,
        out_specs=out_specs,
        compiler_params=pltpu.CompilerParams(vmem_limit_bytes=24 * 1024 * 1024),
    )(*operands)


def shards_any(queries, keys, values, span_order):
    n = lax.axis_size("ctx")
    rows = queries.shape[0]
    k_all = lax.all_gather(keys, "ctx", axis=0, tiled=True)
    v_all = lax.all_gather(values, "ctx", axis=0, tiled=True)
    state = None
    for s in range(n):
        piece = (k_all[s * rows : (s + 1) * rows], v_all[s * rows : (s + 1) * rows])
        state = attend(span_order, queries, [piece], [lambda me, s=s: (s, None)], state, s == n - 1)
    return state


def shards(queries, keys, values, span_order):
    if lax.axis_size("ctx") != 4:
        return shards_any(queries, keys, values, span_order)

    def send(pairs):
        return [lax.ppermute(x, "ctx", pairs) for x in (keys, values)]

    far = send([(0, 2), (2, 0), (1, 3), (3, 1)])
    near = send([(0, 1), (1, 0), (2, 3), (3, 2)])
    cross = send([(0, 3), (3, 0), (1, 2), (2, 1)])
    state = attend(span_order, queries, [(keys, values)], [lambda me: (me, None)], None, False)
    state = attend(
        span_order, queries, [near], [lambda me: (me + 1 - 2 * (me % 2), None)], state, False
    )
    state = attend(span_order, queries, [far], [lambda me: ((me + 2) % 4, None)], state, False)
    return attend(span_order, queries, [cross], [lambda me: (3 - me, None)], state, True)


def solution(mesh):
    spec = P(("groups", "ctx"), ("head", "rep"))
    return jax.shard_map(
        shards,
        mesh=mesh,
        in_specs=(spec, spec, spec, P()),
        out_specs=spec,
        check_vma=False,
    )
```
